32 devices in a mesh: tm: 2 (over y), row: 4 (over z), col: 4 (over x, core).
Axes of the slice: x: 2, y: 2, z: 4, core: 2. Of those that a mesh axis runs over, the one named last changes fastest.
Arguments:
- returns: bfloat16 [272, 16384], P('tm', ('row', 'col')), may hold values from -60 to 60
- window: int32 [1], replicated, may hold values from 200 to 256
- out_days: int32 [4], replicated, may hold values from 255 to 271
Outputs:
- correlation: bfloat16 [4, 16384, 16384], P(None, 'row', ('col', 'tm'))
The draws below stay inside these ranges and needn't reach their ends.
Inputs may be any that keep to these rules, and one draw needn't show every extreme that they name: One window length for all days. `out_days`: days may repeat.
All inputs are finite; a program needn't handle non-finite values.
Results may differ from the reference program's by a relative error of at most 0.001.
Values may be sent and summed in bfloat16 or wider, within the bound.
A program may use at most 128 MiB of HBM per device.

```python
import jax
import jax.numpy as jnp
from jax import lax

ASSETS = 16384
DAYS = 272
NOUT = 4


def draw_returns(key, part):
    keys = jax.random.split(jax.random.fold_in(key, 17), 5)
    day_scale = jnp.exp(jax.random.uniform(keys[0], (DAYS, 1), jnp.float32, jnp.log(0.3), jnp.log(3.0)))
    asset_scale = jnp.exp(jax.random.uniform(keys[1], (1, ASSETS), jnp.float32, jnp.log(0.5), jnp.log(5.0)))
    loading = jax.random.uniform(keys[2], (1, ASSETS), jnp.float32, 0.4, 1.6)
    market = jax.random.normal(keys[3], (DAYS, 1), jnp.float32)
    noise = jax.random.normal(keys[4], (DAYS, ASSETS), jnp.float32)
    signal = loading * market + noise
    values = jnp.clip(day_scale * asset_scale * signal, -60.0, 60.0)
    return values.astype(jnp.bfloat16)


def plant(entries, key, smallest, top_value):
    extent = entries.shape
    place = [jax.random.randint(jax.random.fold_in(key, axis), (), 0, extent[axis]) for axis in range(len(extent))]
    entries = entries.at[tuple(place)].set(smallest)
    longest = extent.index(max(extent))
    place[longest] = (place[longest] + 1) % extent[longest]
    return entries.at[tuple(place)].set(top_value)


def setup_inputs(seed: int = 0) -> dict:
    streams_of = jax.random.split(jax.random.key(seed), 4)
    return {
        "returns": draw_returns(jax.random.fold_in(streams_of[3], 71), 0),
        "window": jax.random.randint(streams_of[1], (1,), 200, 257).astype(jnp.int32),
        "out_days": plant(jax.random.randint(streams_of[2], (NOUT,), 255, DAYS), jax.random.fold_in(streams_of[2], 1), 255, DAYS - 1).astype(jnp.int32),
    }


def reference(returns, window, out_days):
    width = window[0]
    wide = width.astype(jnp.float32)
    day_ids = jnp.arange(DAYS, dtype=jnp.int32)
    inside = (day_ids[None, :] <= out_days[:, None]) & (day_ids[None, :] > out_days[:, None] - width)
    mask = jnp.where(inside, 1.0, 0.0).astype(jnp.float32)
    series = returns.astype(jnp.float32)
    first = jnp.dot(mask, series, precision=lax.Precision.HIGHEST)
    second = jnp.dot(mask, series * series, precision=lax.Precision.HIGHEST)
    scale = lax.rsqrt((second - first * first / wide) / wide + 1e-06)
    blocks = ASSETS // 512

    def one_block(index):
        start = (index * 512).astype(jnp.int32)
        rows = lax.dynamic_slice_in_dim(series, start, 512, 1)
        weighted = mask[:, :, None] * rows[None, :, :]
        gram = jnp.einsum('kda,db->kab', weighted, series, precision=lax.Precision.HIGHEST)
        first_rows = lax.dynamic_slice_in_dim(first, start, 512, 1)
        scale_rows = lax.dynamic_slice_in_dim(scale, start, 512, 1)
        cov = gram - first_rows[:, :, None] * first[:, None, :] / wide
        return (cov * scale_rows[:, :, None] * scale[:, None, :] / wide).astype(jnp.bfloat16)
    pieces = lax.map(one_block, jnp.arange(blocks, dtype=jnp.int32))
    return jnp.transpose(pieces, (1, 0, 2, 3)).reshape(NOUT, ASSETS, ASSETS)
```

```python
import functools

import jax
import jax.numpy as jnp
from jax import lax
from jax.experimental import pallas as pl
from jax.experimental.pallas import tpu as pltpu
from jax.sharding import PartitionSpec as P

MESH = pl.DeviceIdType.MESH


def gather_kernel(T, R, C, S, x_ref, rows_ref, cols_ref, line, line_send, line_recv,
                  row_send, row_recv, twin_send, relay_send, col_send, col_recv, local_sem):
    t, r, c = lax.axis_index("tm"), lax.axis_index("row"), lax.axis_index("col")
    half, width = x_ref.shape
    sub = width // S
    n = R // T
    core = lax.rem(c, 2)
    twin = c + 1 - 2 * core
    chips = C // 2
    chip = c // 2

    def to(tt, rr, cc):
        return {"tm": tt, "row": rr, "col": cc}

    barrier = pltpu.get_barrier_semaphore()
    for d in range(1, T * C):
        flat = lax.rem(t * C + c + d, T * C)
        pl.semaphore_signal(barrier, inc=1, device_id=to(flat // C, r, lax.rem(flat, C)), device_id_type=MESH)

    @pl.when(r > 0)
    def _():
        pl.semaphore_signal(barrier, inc=1, device_id=to(t, r - 1, c), device_id_type=MESH)

    @pl.when(r < R - 1)
    def _():
        pl.semaphore_signal(barrier, inc=1, device_id=to(t, r + 1, c), device_id_type=MESH)

    inner = jnp.logical_and(r > 0, r < R - 1)
    pl.semaphore_wait(barrier, T * C + inner.astype(jnp.int32) if R > 1 else T * C - 1)

    def rdma(src, dst, send, recv, device):
        return pltpu.make_async_remote_copy(src_ref=src, dst_ref=dst, send_sem=send, recv_sem=recv,
                                            device_id=device, device_id_type=MESH)

    def part(s):
        return x_ref.at[:, pl.ds(s * sub, sub)]

    def row_slot(tt, cc, s):
        return rows_ref.at[pl.ds(pl.multiple_of(tt * half, 8), half),
                           pl.ds(pl.multiple_of(cc * width + s * sub, sub), sub)]

    def col_slot(tt, j, s):
        return cols_ref.at[pl.ds(pl.multiple_of(tt * half, 8), half),
                           pl.ds(pl.multiple_of(j * width + s * sub, sub), sub)]

    def line_copy(src, q, s, up):
        return rdma(src, line.at[q, s], line_send.at[int(up), q, s], line_recv.at[q, s],
                    to(t, r + (1 if up else -1), c))

    def send_line(src, q, s, up):
        ok = (r < R - 1) if up else (r > 0)

        @pl.when(ok)
        def _():
            line_copy(src, q, s, up).start()

    def col_place(q):
        piece = q * C + c
        group = piece // n
        return lax.rem(group, T), group // T, lax.rem(piece, n)

    def col_copy(src, q, s):
        tt, cc, j = col_place(q)
        return rdma(src, col_slot(t, j, s), col_send.at[q, s], col_recv.at[t, j, s], to(tt, r, cc))

    def send_col(src, q, s):
        tt, cc, j = col_place(q)
        mine = jnp.logical_and(tt == t, cc == c)

        @pl.when(mine)
        def _():
            pltpu.make_async_copy(src, col_slot(t, j, s), col_recv.at[t, j, s]).start()

        @pl.when(jnp.logical_not(mine))
        def _():
            col_copy(src, q, s).start()

    near = [(dt, dx) for dt in range(T) for dx in range(chips) if dt or dx]
    far = []

    def at_chip(dt, dx):
        return lax.rem(t + dt + T, T), 2 * lax.rem(chip + dx + chips, chips) + core

    def own_copy(i, s):
        tt, cc = at_chip(*near[i])
        return rdma(part(s), row_slot(t, c, s), row_send.at[i, s], row_recv.at[t, c, s], to(tt, r, cc))

    def own_twin(s):
        return rdma(part(s), row_slot(t, c, s), row_send.at[len(near), s], row_recv.at[t, c, s], to(t, r, twin))

    def twin_copy(dt, dx, s):
        tt, cc = at_chip(-dt, -dx)
        slot = row_slot(tt, cc, s)
        return rdma(slot, slot, twin_send.at[dt, dx, s], row_recv.at[tt, cc, s], to(t, r, twin))

    def relays(dt, dx):
        if dt == 0:
            return core == 0, [(d, 0) for d in range(1, T)]
        return core == 1, [(0, d) for d in range(1, chips)]

    def relay_copy(dt, dx, hop, s):
        tt, cc = at_chip(-dt, -dx)
        slot = row_slot(tt, cc, s)
        ht, hc = at_chip(*hop)
        return rdma(slot, slot, relay_send.at[dt, dx, max(hop) - 1, s], row_recv.at[tt, cc, s], to(ht, r, hc))

    def row_arrived(dt, dx, s):
        twin_copy(dt, dx, s).wait_recv()
        if False:
            ok, hops = relays(dt, dx)

            @pl.when(ok)
            def _():
                for hop in hops:
                    relay_copy(dt, dx, hop, s).start()
        twin_copy(dt, dx, s).start()

    def line_arrived(dist, s):
        for up in (True, False):
            q = r - dist if up else r + dist
            ok = (q >= 0) if up else (q < R)

            @pl.when(ok)
            def _():
                line_copy(line.at[q, s], q, s, up).wait_recv()
                send_line(line.at[q, s], q, s, up)
                send_col(line.at[q, s], q, s)

    own_out = pltpu.make_async_copy(x_ref, rows_ref.at[pl.ds(pl.multiple_of(t * half, 8), half),
                                                       pl.ds(pl.multiple_of(c * width, width), width)], local_sem)
    for s in range(S):
        send_line(part(s), r, s, True)
        send_line(part(s), r, s, False)
    for s in range(S):
        for i in range(len(near)):
            own_copy(i, s).start()
    for s in range(S):
        own_twin(s).start()
        send_col(part(s), r, s)
    own_out.start()

    for dist in range(1, R):
        for s in range(S):
            line_arrived(dist, s)
            if dist == min(2, R - 1) and s == S - 1:
                for s2 in range(S):
                    for dt, dx in near:
                        row_arrived(dt, dx, s2)
            if dist == min(2, R - 1):
                for dt, dx in far:
                    row_arrived(dt, dx, s)

    own_out.wait()
    for s in range(S):
        for i in range(len(near)):
            own_copy(i, s).wait_send()
        own_twin(s).wait_send()
        own_twin_slot = row_slot(t, twin, s)
        rdma(own_twin_slot, own_twin_slot, row_send.at[len(near), s], row_recv.at[t, twin, s], to(t, r, twin)).wait_recv()
        for dt, dx in near + far:
            twin_copy(dt, dx, s).wait_send()
            tt, cc = at_chip(-dt, -dx)
            theirs = row_slot(tt, cc + 1 - 2 * core, s)
            rdma(theirs, theirs, twin_send.at[dt, dx, s], row_recv.at[tt, cc + 1 - 2 * core, s], to(t, r, twin)).wait_recv()
    for s in range(S):
        for tt in range(T):
            for j in range(n):
                slot = col_slot(tt, j, s)
                pltpu.make_async_copy(slot, slot, col_recv.at[tt, j, s]).wait()
        for q in range(R):
            tt, cc, j = col_place(q)

            @pl.when(jnp.logical_not(jnp.logical_and(tt == t, cc == c)))
            def _():
                col_copy(part(s), q, s).wait_send()

            @pl.when(jnp.logical_and(q <= r, r < R - 1))
            def _():
                line_copy(part(s), q, s, True).wait_send()

            @pl.when(jnp.logical_and(q >= r, r > 0))
            def _():
                line_copy(part(s), q, s, False).wait_send()


def gather(returns, T, R, C, S=2):
    half, width = returns.shape
    n = R // T
    S = S if width % (128 * S) == 0 else 1
    sub = width // S
    dma = pltpu.SemaphoreType.DMA
    chips = C // 2
    near = T * chips - 1
    dt = returns.dtype
    return pl.pallas_call(
        functools.partial(gather_kernel, T, R, C, S),
        out_shape=(
            jax.ShapeDtypeStruct((T * half, C * width), dt),
            jax.ShapeDtypeStruct((T * half, n * width), dt),
        ),
        in_specs=[pl.BlockSpec(memory_space=pltpu.VMEM)],
        out_specs=(pl.BlockSpec(memory_space=pl.ANY), pl.BlockSpec(memory_space=pl.ANY)),
        scratch_shapes=[
            pltpu.VMEM((R, S, half, sub), dt),
            dma((2, R, S)), dma((R, S)),
            dma((near + 1, S)), dma((T, C, S)), dma((T, chips, S)), dma((T, chips, max(T, chips), S)),
            dma((R, S)), dma((T, n, S)), dma,
        ],
        compiler_params=pltpu.CompilerParams(collective_id=0, has_side_effects=True),
    )(returns)


DEPTH = 256
FOLD = 6
BF = jnp.bfloat16
F32 = jnp.float32


def split3(v):
    hi = v.astype(BF).astype(F32)
    mid = (v - hi).astype(BF).astype(F32)
    return hi, mid, v - hi - mid


def indicator(cond):
    return jnp.where(cond, 1.0, 0.0).astype(BF)


def wide_mask(m, width):
    return jnp.concatenate([m] * (width // 128), axis=1)


def corr_kernel(tile, chunk, window_ref, days_ref, row_ref, col_ref, out_ref,
                row_head, row_rest, col_head, col_a, col_m, row_stat, obuf, sems):
    K = days_ref.shape[0]
    days, M = row_ref.shape
    N = col_ref.shape[1]
    extra = days - DEPTH
    w = window_ref[0]
    wide = w.astype(F32)
    recip = 1.0 / wide
    fold = w <= DEPTH - FOLD

    kk = lax.broadcasted_iota(jnp.int32, (16, days), 0)
    day = lax.broadcasted_iota(jnp.int32, (16, days), 1)
    lasts = jnp.full((16, days), -1, jnp.int32)
    for k in range(K):
        lasts = jnp.where(kk == k, days_ref[k], lasts)
    inside = indicator((day <= lasts) & (day > lasts - w))

    slot = lax.broadcasted_iota(jnp.int32, (16, 128), 0)

    def stats(x):
        xf = x.astype(F32)
        sq = xf * xf
        hi = sq.astype(BF)
        lo = (sq - hi.astype(F32)).astype(BF)
        dot = functools.partial(jnp.dot, preferred_element_type=F32)
        first = dot(inside, x)
        second = dot(inside, hi) + dot(inside, lo)
        scale = lax.rsqrt((second - first * first / wide) / wide + 1e-06)
        return first, scale

    def masks(k):
        last = days_ref[k]
        base = last - (DEPTH - 1)
        per_block = []
        for blk in range(128 // 16):
            s = slot + 16 * blk
            keep = indicator((s > last - w) & (s + DEPTH > last))if blk == 0 else indicator(s > last - w)
            if 16 * blk <= extra + FOLD - 1:
                n = s - base
                hi = indicator(fold & ((n == 0) | (n == 1) | (n == 4)))
                mid = indicator(fold & ((n == 2) | (n == 3)))
                low = indicator(fold & (n == 5))
                other = indicator(fold & ((n == 0) | (n == 2) | (n == 5)))
                other_mid = indicator(fold & ((n == 1) | (n == 3)))
                other_low = indicator(fold & (n == 4))
                per_block.append((keep, (hi, mid, low), (other, other_mid, other_low)))
            else:
                per_block.append((keep, None, None))
        late = indicator(slot + DEPTH <= last)
        return per_block, late

    def head_of(k, x, value, side):
        width = x.shape[1]
        per_block, late = masks(k)
        parts = [jnp.broadcast_to(p[k:k + 1], (16, width)).astype(BF) for p in value]
        blocks = []
        for blk, mk in enumerate(per_block):
            v = x[16 * blk:16 * blk + 16] * wide_mask(mk[0], width)
            if blk == 0:
                v = v + x[DEPTH:] * wide_mask(late, width)
            if mk[1] is not None:
                for p, m in zip(parts, mk[1 + side]):
                    v = v + p * wide_mask(m, width)
            blocks.append(v)
        return jnp.concatenate(blocks, axis=0)

    for c0 in range(0, N, chunk):
        at = pl.ds(c0, chunk)
        x = col_ref[:, at]
        first, scale = stats(x)
        a = scale * recip
        m = first * recip * a
        parts = split3(first)
        for k in range(K):
            col_a[k, :, at] = a[k:k + 1]
            col_m[k, :, at] = m[k:k + 1]
            col_head[k, :, at] = head_of(k, x, parts, 1)

    for c0 in range(0, M, chunk):
        at = pl.ds(c0, chunk)
        x = row_ref[:, at]
        first, scale = stats(x)
        both = jnp.concatenate([scale[:8], (first * scale)[:8]], axis=0)
        pad = jnp.concatenate([both, jnp.zeros((112, chunk), F32)], axis=0)
        row_stat[at, :] = pad.T
        parts = split3(-first * recip)
        for k in range(K):
            row_head[k, at, :] = head_of(k, x, parts, 0).T
        row_rest[at, :] = x[128:DEPTH].T

    step = 256 if N % 256 == 0 else 128
    G = M // tile

    def copy_out(i, k):
        b = lax.rem(i, 2)
        return pltpu.make_async_copy(obuf.at[b, k], out_ref.at[k, pl.ds(pl.multiple_of(i * tile, tile), tile), :],
                                     sems.at[b, k])

    def run(folded):
        def body(i, carry):
            b = lax.rem(i, 2)

            @pl.when(i >= 2)
            def _():
                for k in range(K):
                    copy_out(i - 2, k).wait()
            at = pl.ds(pl.multiple_of(i * tile, tile), tile)
            for k in range(K):
                lhs = jnp.concatenate([row_head[k, at, :], row_rest[at, :]], axis=1)
                s = jnp.broadcast_to(row_stat[at, k:k + 1], (tile, 128))
                s = jnp.concatenate([s] * (step // 128), axis=1)
                if not folded:
                    m = jnp.broadcast_to(row_stat[at, 8 + k:9 + k], (tile, 128))
                    m = jnp.concatenate([m] * (step // 128), axis=1)
                for j in range(0, N, step):
                    rhs = jnp.concatenate([col_head[k, :, j:j + step], col_ref[128:DEPTH, j:j + step]], axis=0)
                    g = jnp.dot(lhs, rhs, preferred_element_type=F32)
                    o = (g * s) * col_a[k, :, j:j + step]
                    if not folded:
                        o = o - m * col_m[k, :, j:j + step]
                    obuf[b, k, :, j:j + step] = o.astype(BF)
                copy_out(i, k).start()
            return carry

        lax.fori_loop(0, G, body, 0)

    @pl.when(fold)
    def _():
        run(True)

    @pl.when(jnp.logical_not(fold))
    def _():
        run(False)

    for i in range(max(0, G - 2), G):
        for k in range(K):
            copy_out(i, k).wait()


def correlate(window, out_days, rows, cols, tile=512, chunk=512):
    days, M = rows.shape
    N = cols.shape[1]
    K = out_days.shape[0]
    tile = min(tile, M)
    chunk = min(chunk, N, M)
    smem = pl.BlockSpec(memory_space=pltpu.SMEM)
    vmem = pl.BlockSpec(memory_space=pltpu.VMEM)
    return pl.pallas_call(
        functools.partial(corr_kernel, tile, chunk),
        out_shape=jax.ShapeDtypeStruct((K, M, N), BF),
        in_specs=[smem, smem, vmem, vmem],
        out_specs=pl.BlockSpec(memory_space=pl.ANY),
        scratch_shapes=[
            pltpu.VMEM((K, M, 128), BF),
            pltpu.VMEM((M, 128), BF),
            pltpu.VMEM((K, 128, N), BF),
            pltpu.VMEM((K, 1, N), F32),
            pltpu.VMEM((K, 1, N), F32),
            pltpu.VMEM((M, 128), F32),
            pltpu.VMEM((2, K, tile, N), BF),
            pltpu.SemaphoreType.DMA((2, K)),
        ],
        compiler_params=pltpu.CompilerParams(vmem_limit_bytes=60 * 2**20),
    )(window, out_days, rows, cols)


def on_device(returns, window, out_days):
    T, R, C = lax.axis_size("tm"), lax.axis_size("row"), lax.axis_size("col")
    rows, cols = gather(returns, T, R, C)
    return correlate(window, out_days, rows, cols)


def solution(mesh):
    return jax.shard_map(
        on_device,
        mesh=mesh,
        in_specs=(P("tm", ("row", "col")), P(), P()),
        out_specs=P(None, "row", ("col", "tm")),
        check_vma=False,
    )
```

```python
import functools

import jax
import jax.numpy as jnp
from jax import lax
from jax.experimental import pallas as pl
from jax.experimental.pallas import tpu as pltpu
from jax.sharding import PartitionSpec as P

MESH = pl.DeviceIdType.MESH


def gather_kernel(T, R, C, S, x_ref, rows_ref, cols_ref, line, line_send, line_recv,
                  row_send, row_recv, twin_send, relay_send, col_send, col_recv, local_sem):
    t, r, c = lax.axis_index("tm"), lax.axis_index("row"), lax.axis_index("col")
    half, width = x_ref.shape
    sub = width // S
    n = R // T
    core = lax.rem(c, 2)
    twin = c + 1 - 2 * core
    chips = C // 2
    chip = c // 2

    def to(tt, rr, cc):
        return {"tm": tt, "row": rr, "col": cc}

    barrier = pltpu.get_barrier_semaphore()
    for d in range(1, T * C):
        flat = lax.rem(t * C + c + d, T * C)
        pl.semaphore_signal(barrier, inc=1, device_id=to(flat // C, r, lax.rem(flat, C)), device_id_type=MESH)

    @pl.when(r > 0)
    def _():
        pl.semaphore_signal(barrier, inc=1, device_id=to(t, r - 1, c), device_id_type=MESH)

    @pl.when(r < R - 1)
    def _():
        pl.semaphore_signal(barrier, inc=1, device_id=to(t, r + 1, c), device_id_type=MESH)

    inner = jnp.logical_and(r > 0, r < R - 1)
    pl.semaphore_wait(barrier, T * C + inner.astype(jnp.int32) if R > 1 else T * C - 1)

    def rdma(src, dst, send, recv, device):
        return pltpu.make_async_remote_copy(src_ref=src, dst_ref=dst, send_sem=send, recv_sem=recv,
                                            device_id=device, device_id_type=MESH)

    def part(s):
        return x_ref.at[:, pl.ds(s * sub, sub)]

    def row_slot(tt, cc, s):
        return rows_ref.at[pl.ds(pl.multiple_of(tt * half, 8), half),
                           pl.ds(pl.multiple_of(cc * width + s * sub, sub), sub)]

    def col_slot(tt, j, s):
        return cols_ref.at[pl.ds(pl.multiple_of(tt * half, 8), half),
                           pl.ds(pl.multiple_of(j * width + s * sub, sub), sub)]

    def line_copy(src, q, s, up):
        return rdma(src, line.at[q, s], line_send.at[int(up), q, s], line_recv.at[q, s],
                    to(t, r + (1 if up else -1), c))

    def send_line(src, q, s, up):
        ok = (r < R - 1) if up else (r > 0)

        @pl.when(ok)
        def _():
            line_copy(src, q, s, up).start()

    def col_place(q):
        piece = q * C + c
        group = piece // n
        return lax.rem(group, T), group // T, lax.rem(piece, n)

    def col_copy(src, q, s):
        tt, cc, j = col_place(q)
        return rdma(src, col_slot(t, j, s), col_send.at[q, s], col_recv.at[t, j, s], to(tt, r, cc))

    def send_col(src, q, s):
        tt, cc, j = col_place(q)
        mine = jnp.logical_and(tt == t, cc == c)

        @pl.when(mine)
        def _():
            pltpu.make_async_copy(src, col_slot(t, j, s), col_recv.at[t, j, s]).start()

        @pl.when(jnp.logical_not(mine))
        def _():
            col_copy(src, q, s).start()

    near = [(dt, dx) for dt in range(T) for dx in range(chips) if dt or dx]
    far = []

    def at_chip(dt, dx):
        return lax.rem(t + dt + T, T), 2 * lax.rem(chip + dx + chips, chips) + core

    def own_copy(i, s):
        tt, cc = at_chip(*near[i])
        return rdma(part(s), row_slot(t, c, s), row_send.at[i, s], row_recv.at[t, c, s], to(tt, r, cc))

    def own_twin(s):
        return rdma(part(s), row_slot(t, c, s), row_send.at[len(near), s], row_recv.at[t, c, s], to(t, r, twin))

    def twin_copy(dt, dx, s):
        tt, cc = at_chip(-dt, -dx)
        slot = row_slot(tt, cc, s)
        return rdma(slot, slot, twin_send.at[dt, dx, s], row_recv.at[tt, cc, s], to(t, r, twin))

    def relays(dt, dx):
        if dt == 0:
            return core == 0, [(d, 0) for d in range(1, T)]
        return core == 1, [(0, d) for d in range(1, chips)]

    def relay_copy(dt, dx, hop, s):
        tt, cc = at_chip(-dt, -dx)
        slot = row_slot(tt, cc, s)
        ht, hc = at_chip(*hop)
        return rdma(slot, slot, relay_send.at[dt, dx, max(hop) - 1, s], row_recv.at[tt, cc, s], to(ht, r, hc))

    def row_arrived(dt, dx, s):
        twin_copy(dt, dx, s).wait_recv()
        if False:
            ok, hops = relays(dt, dx)

            @pl.when(ok)
            def _():
                for hop in hops:
                    relay_copy(dt, dx, hop, s).start()
        twin_copy(dt, dx, s).start()

    def line_arrived(dist, s):
        for up in (True, False):
            q = r - dist if up else r + dist
            ok = (q >= 0) if up else (q < R)

            @pl.when(ok)
            def _():
                line_copy(line.at[q, s], q, s, up).wait_recv()
                send_line(line.at[q, s], q, s, up)
                send_col(line.at[q, s], q, s)

    own_out = pltpu.make_async_copy(x_ref, rows_ref.at[pl.ds(pl.multiple_of(t * half, 8), half),
                                                       pl.ds(pl.multiple_of(c * width, width), width)], local_sem)
    for s in range(S):
        send_line(part(s), r, s, True)
        send_line(part(s), r, s, False)
    for s in range(S):
        for i in range(len(near)):
            own_copy(i, s).start()
    for s in range(S):
        own_twin(s).start()
        send_col(part(s), r, s)
    own_out.start()

    for dist in range(1, R):
        for s in range(S):
            line_arrived(dist, s)
            if dist == min(2, R - 1) and s == S - 1:
                for s2 in range(S):
                    for dt, dx in near:
                        row_arrived(dt, dx, s2)
            if dist == min(2, R - 1):
                for dt, dx in far:
                    row_arrived(dt, dx, s)

    own_out.wait()
    for s in range(S):
        for i in range(len(near)):
            own_copy(i, s).wait_send()
        own_twin(s).wait_send()
        own_twin_slot = row_slot(t, twin, s)
        rdma(own_twin_slot, own_twin_slot, row_send.at[len(near), s], row_recv.at[t, twin, s], to(t, r, twin)).wait_recv()
        for dt, dx in near + far:
            twin_copy(dt, dx, s).wait_send()
            tt, cc = at_chip(-dt, -dx)
            theirs = row_slot(tt, cc + 1 - 2 * core, s)
            rdma(theirs, theirs, twin_send.at[dt, dx, s], row_recv.at[tt, cc + 1 - 2 * core, s], to(t, r, twin)).wait_recv()
    for s in range(S):
        for tt in range(T):
            for j in range(n):
                slot = col_slot(tt, j, s)
                pltpu.make_async_copy(slot, slot, col_recv.at[tt, j, s]).wait()
        for q in range(R):
            tt, cc, j = col_place(q)

            @pl.when(jnp.logical_not(jnp.logical_and(tt == t, cc == c)))
            def _():
                col_copy(part(s), q, s).wait_send()

            @pl.when(jnp.logical_and(q <= r, r < R - 1))
            def _():
                line_copy(part(s), q, s, True).wait_send()

            @pl.when(jnp.logical_and(q >= r, r > 0))
            def _():
                line_copy(part(s), q, s, False).wait_send()


def gather(returns, T, R, C, S=2):
    half, width = returns.shape
    n = R // T
    S = S if width % (128 * S) == 0 else 1
    sub = width // S
    dma = pltpu.SemaphoreType.DMA
    chips = C // 2
    near = T * chips - 1
    dt = returns.dtype
    return pl.pallas_call(
        functools.partial(gather_kernel, T, R, C, S),
        out_shape=(
            jax.ShapeDtypeStruct((T * half, C * width), dt),
            jax.ShapeDtypeStruct((T * half, n * width), dt),
        ),
        in_specs=[pl.BlockSpec(memory_space=pltpu.VMEM)],
        out_specs=(pl.BlockSpec(memory_space=pl.ANY), pl.BlockSpec(memory_space=pl.ANY)),
        scratch_shapes=[
            pltpu.VMEM((R, S, half, sub), dt),
            dma((2, R, S)), dma((R, S)),
            dma((near + 1, S)), dma((T, C, S)), dma((T, chips, S)), dma((T, chips, max(T, chips), S)),
            dma((R, S)), dma((T, n, S)), dma,
        ],
        compiler_params=pltpu.CompilerParams(collective_id=0, has_side_effects=True),
    )(returns)


DEPTH = 256
FOLD = 6
BF = jnp.bfloat16
F32 = jnp.float32


def split3(v):
    hi = v.astype(BF).astype(F32)
    mid = (v - hi).astype(BF).astype(F32)
    return hi, mid, v - hi - mid


def indicator(cond):
    return jnp.where(cond, 1.0, 0.0).astype(BF)


def wide_mask(m, width):
    return jnp.concatenate([m] * (width // 128), axis=1)


def corr_kernel(tile, chunk, window_ref, days_ref, rows_hbm, cols_hbm, out_ref,
                row_ref, col_ref, mask_ref, head_a, rest_a, head_b, rest_b,
                row_stat, row_p, col_head, col_a, col_m, obuf, sems, load_sems):
    K = days_ref.shape[0]
    days, M = row_ref.shape
    N = col_ref.shape[1]
    extra = days - DEPTH
    heads = 128 // 16
    w = window_ref[0]
    wide = w.astype(F32)
    recip = 1.0 / wide
    fold = w <= DEPTH - FOLD
    load_cols = pltpu.make_async_copy(cols_hbm, col_ref, load_sems.at[0])
    load_rows = pltpu.make_async_copy(rows_hbm, row_ref, load_sems.at[1])
    load_cols.start()
    load_rows.start()

    kk = lax.broadcasted_iota(jnp.int32, (16, days), 0)
    day = lax.broadcasted_iota(jnp.int32, (16, days), 1)
    lasts = jnp.full((16, days), -1, jnp.int32)
    for k in range(K):
        lasts = jnp.where(kk == k, days_ref[k], lasts)
    inside = indicator((day <= lasts) & (day > lasts - w))

    slot = lax.broadcasted_iota(jnp.int32, (16, 128), 0)
    folded_blocks = (extra + FOLD - 1) // 16 + 1

    for k in range(K):
        last = days_ref[k]
        for blk in range(heads):
            s = slot + 16 * blk
            keep = s > last - w
            if blk == 0:
                keep = keep & (s + DEPTH > last)
            mask_ref[k, blk] = indicator(keep)
        mask_ref[k, heads] = indicator(slot + DEPTH <= last)
        for blk in range(folded_blocks):
            n = slot + 16 * blk - (last - (DEPTH - 1))
            sets = ((0, 1, 4), (2, 3), (5,), (0, 2, 5), (1, 3), (4,))
            for e, members in enumerate(sets):
                hit = functools.reduce(jnp.logical_or, [n == v for v in members])
                mask_ref[k, heads + 1 + 6 * blk + e] = indicator(fold & hit)

    def stats(x):
        xf = x.astype(F32)
        sq = xf * xf
        hi = sq.astype(BF)
        lo = (sq - hi.astype(F32)).astype(BF)
        dot = functools.partial(jnp.dot, preferred_element_type=F32)
        first = dot(inside, x)
        second = dot(inside, hi) + dot(inside, lo)
        scale = lax.rsqrt((second - first * first / wide) / wide + 1e-06)
        return first, scale

    def head_of(k, x, value, side):
        width = x.shape[1]
        parts = [jnp.broadcast_to(p[k:k + 1], (16, width)).astype(BF) for p in value]
        blocks = []
        for blk in range(heads):
            v = x[16 * blk:16 * blk + 16] * wide_mask(mask_ref[k, blk], width)
            if blk == 0:
                v = v + x[DEPTH:] * wide_mask(mask_ref[k, heads], width)
            if blk < folded_blocks:
                for e, p in enumerate(parts):
                    v = v + p * wide_mask(mask_ref[k, heads + 1 + 6 * blk + 3 * side + e], width)
            blocks.append(v)
        return jnp.concatenate(blocks, axis=0)

    load_cols.wait()
    for c0 in range(0, N, chunk):
        at = pl.ds(c0, chunk)
        x = col_ref[:, at]
        first, scale = stats(x)
        a = scale * recip
        m = first * recip * a
        parts = split3(first)
        for k in range(K):
            col_a[k, :, at] = a[k:k + 1]
            col_m[k, :, at] = m[k:k + 1]
            col_head[k, :, at] = head_of(k, x, parts, 1)
    load_rows.wait()

    for c0 in range(0, M, chunk):
        at = pl.ds(c0, chunk)
        first, scale = stats(row_ref[:, at])
        row_p[:, at] = (-first * recip)[:8]
        both = jnp.concatenate([scale[:8], (first * scale)[:8]], axis=0)
        row_stat[at, :] = jnp.concatenate([both, jnp.zeros((112, chunk), F32)], axis=0).T

    def prepare(i, refs):
        head, rest = refs
        at = pl.ds(pl.multiple_of(i * tile, tile), tile)
        x = row_ref[:, at]
        parts = split3(row_p[:, at])
        for k in range(K):
            head[k] = head_of(k, x, parts, 0).T
            if k == K - 1:
                rest[...] = x[128:DEPTH].T
            yield

    step = 256 if N % 256 == 0 else 128
    G = M // tile

    span = N // 2 if N % (2 * step) == 0 else N
    pieces = range(N // span)

    def copy_out(i, b, k, h):
        at = pl.ds(h * span, span)
        return pltpu.make_async_copy(obuf.at[b, k, :, at],
                                     out_ref.at[k, pl.ds(pl.multiple_of(i * tile, tile), tile), at],
                                     sems.at[b, k, h])

    def multiply(i, b, refs, folded, stages):
        head, rest = refs
        at = pl.ds(pl.multiple_of(i * tile, tile), tile)
        for k in range(K):
            lhs = jnp.concatenate([head[k], rest[...]], axis=1)
            s = jnp.broadcast_to(row_stat[at, k:k + 1], (tile, 128))
            s = jnp.concatenate([s] * (step // 128), axis=1)
            if not folded:
                m = jnp.broadcast_to(row_stat[at, 8 + k:9 + k], (tile, 128))
                m = jnp.concatenate([m] * (step // 128), axis=1)
            for j in range(0, N, step):
                rhs = jnp.concatenate([col_head[k, :, j:j + step], col_ref[128:DEPTH, j:j + step]], axis=0)
                g = jnp.dot(lhs, rhs, preferred_element_type=F32)
                o = (g * s) * col_a[k, :, j:j + step]
                if not folded:
                    o = o - m * col_m[k, :, j:j + step]
                obuf[b, k, :, j:j + step] = o.astype(BF)
                if (j + step) % span == 0:
                    copy_out(i, b, k, j // span).start()
            next(stages, None)
        for _ in stages:
            pass

    first_refs = (head_a, rest_a)
    second_refs = (head_b, rest_b)
    for _ in prepare(0, first_refs):
        pass

    def run(folded):
        def body(p, carry):
            for b, (now, later) in enumerate(((first_refs, second_refs), (second_refs, first_refs))):
                i = 2 * p + b

                @pl.when(p > 0)
                def _():
                    for k in range(K):
                        for h in pieces:
                            copy_out(i - 2, b, k, h).wait()
                multiply(i, b, now, folded, prepare(jnp.minimum(i + 1, G - 1), later))
            return carry

        lax.fori_loop(0, G // 2, body, 0)

    @pl.when(fold)
    def _():
        run(True)

    @pl.when(jnp.logical_not(fold))
    def _():
        run(False)

    for b in range(2):
        for k in range(K):
            for h in pieces:
                copy_out(G - 2 + b, b, k, h).wait()


def correlate(window, out_days, rows, cols, tile=512, chunk=512):
    days, M = rows.shape
    N = cols.shape[1]
    K = out_days.shape[0]
    tile = min(tile, M // 2)
    chunk = min(chunk, N, M)
    folded_blocks = (days - DEPTH + FOLD - 1) // 16 + 1
    smem = pl.BlockSpec(memory_space=pltpu.SMEM)
    hbm = pl.BlockSpec(memory_space=pl.ANY)
    side = [pltpu.VMEM((K, tile, 128), BF), pltpu.VMEM((tile, 128), BF)]
    return pl.pallas_call(
        functools.partial(corr_kernel, tile, chunk),
        out_shape=jax.ShapeDtypeStruct((K, M, N), BF),
        in_specs=[smem, smem, hbm, hbm],
        out_specs=hbm,
        scratch_shapes=[
            pltpu.VMEM((days, M), BF),
            pltpu.VMEM((days, N), BF),
            pltpu.VMEM((K, 9 + 6 * folded_blocks, 16, 128), BF),
            *side, *side,
            pltpu.VMEM((M, 128), F32),
            pltpu.VMEM((8, M), F32),
            pltpu.VMEM((K, 128, N), BF),
            pltpu.VMEM((K, 1, N), F32),
            pltpu.VMEM((K, 1, N), F32),
            pltpu.VMEM((2, K, tile, N), BF),
            pltpu.SemaphoreType.DMA((2, K, 2)),
            pltpu.SemaphoreType.DMA((2,)),
        ],
        compiler_params=pltpu.CompilerParams(vmem_limit_bytes=60 * 2**20),
    )(window, out_days, rows, cols)


def on_device(returns, window, out_days):
    T, R, C = lax.axis_size("tm"), lax.axis_size("row"), lax.axis_size("col")
    rows, cols = gather(returns, T, R, C)
    return correlate(window, out_days, rows, cols)


def solution(mesh):
    return jax.shard_map(
        on_device,
        mesh=mesh,
        in_specs=(P("tm", ("row", "col")), P(), P()),
        out_specs=P(None, "row", ("col", "tm")),
        check_vma=False,
    )
```

```python
import functools

import jax
import jax.numpy as jnp
from jax import lax
from jax.experimental import pallas as pl
from jax.experimental.pallas import tpu as pltpu
from jax.sharding import PartitionSpec as P

MESH = pl.DeviceIdType.MESH


def gather_kernel(T, R, C, S, x_ref, rows_ref, cols_ref, line, line_send, line_recv,
                  row_send, row_recv, twin_send, relay_send, col_send, col_recv, local_sem):
    t, r, c = lax.axis_index("tm"), lax.axis_index("row"), lax.axis_index("col")
    half, width = x_ref.shape
    sub = width // S
    n = R // T
    core = lax.rem(c, 2)
    twin = c + 1 - 2 * core
    chips = C // 2
    chip = c // 2

    def to(tt, rr, cc):
        return {"tm": tt, "row": rr, "col": cc}

    barrier = pltpu.get_barrier_semaphore()
    for d in range(1, T * C):
        flat = lax.rem(t * C + c + d, T * C)
        pl.semaphore_signal(barrier, inc=1, device_id=to(flat // C, r, lax.rem(flat, C)), device_id_type=MESH)

    @pl.when(r > 0)
    def _():
        pl.semaphore_signal(barrier, inc=1, device_id=to(t, r - 1, c), device_id_type=MESH)

    @pl.when(r < R - 1)
    def _():
        pl.semaphore_signal(barrier, inc=1, device_id=to(t, r + 1, c), device_id_type=MESH)

    inner = jnp.logical_and(r > 0, r < R - 1)
    pl.semaphore_wait(barrier, T * C + inner.astype(jnp.int32) if R > 1 else T * C - 1)

    def rdma(src, dst, send, recv, device):
        return pltpu.make_async_remote_copy(src_ref=src, dst_ref=dst, send_sem=send, recv_sem=recv,
                                            device_id=device, device_id_type=MESH)

    def part(s):
        return x_ref.at[:, pl.ds(s * sub, sub)]

    def row_slot(tt, cc, s):
        return rows_ref.at[pl.ds(pl.multiple_of(tt * half, 8), half),
                           pl.ds(pl.multiple_of(cc * width + s * sub, sub), sub)]

    def col_slot(tt, j, s):
        return cols_ref.at[pl.ds(pl.multiple_of(tt * half, 8), half),
                           pl.ds(pl.multiple_of(j * width + s * sub, sub), sub)]

    def line_copy(src, q, s, up):
        return rdma(src, line.at[q, s], line_send.at[int(up), q, s], line_recv.at[q, s],
                    to(t, r + (1 if up else -1), c))

    def send_line(src, q, s, up):
        ok = (r < R - 1) if up else (r > 0)

        @pl.when(ok)
        def _():
            line_copy(src, q, s, up).start()

    def col_place(q):
        piece = q * C + c
        group = piece // n
        return lax.rem(group, T), group // T, lax.rem(piece, n)

    def col_copy(src, q, s):
        tt, cc, j = col_place(q)
        return rdma(src, col_slot(t, j, s), col_send.at[q, s], col_recv.at[t, j, s], to(tt, r, cc))

    def send_col(src, q, s):
        tt, cc, j = col_place(q)
        mine = jnp.logical_and(tt == t, cc == c)

        @pl.when(mine)
        def _():
            pltpu.make_async_copy(src, col_slot(t, j, s), col_recv.at[t, j, s]).start()

        @pl.when(jnp.logical_not(mine))
        def _():
            col_copy(src, q, s).start()

    near = [(dt, dx) for dt in range(T) for dx in range(chips) if dt or dx]
    far = []

    def at_chip(dt, dx):
        return lax.rem(t + dt + T, T), 2 * lax.rem(chip + dx + chips, chips) + core

    def own_copy(i, s):
        tt, cc = at_chip(*near[i])
        return rdma(part(s), row_slot(t, c, s), row_send.at[i, s], row_recv.at[t, c, s], to(tt, r, cc))

    def own_twin(s):
        return rdma(part(s), row_slot(t, c, s), row_send.at[len(near), s], row_recv.at[t, c, s], to(t, r, twin))

    def twin_copy(dt, dx, s):
        tt, cc = at_chip(-dt, -dx)
        slot = row_slot(tt, cc, s)
        return rdma(slot, slot, twin_send.at[dt, dx, s], row_recv.at[tt, cc, s], to(t, r, twin))

    def relays(dt, dx):
        if dt == 0:
            return core == 0, [(d, 0) for d in range(1, T)]
        return core == 1, [(0, d) for d in range(1, chips)]

    def relay_copy(dt, dx, hop, s):
        tt, cc = at_chip(-dt, -dx)
        slot = row_slot(tt, cc, s)
        ht, hc = at_chip(*hop)
        return rdma(slot, slot, relay_send.at[dt, dx, max(hop) - 1, s], row_recv.at[tt, cc, s], to(ht, r, hc))

    def row_arrived(dt, dx, s):
        twin_copy(dt, dx, s).wait_recv()
        if False:
            ok, hops = relays(dt, dx)

            @pl.when(ok)
            def _():
                for hop in hops:
                    relay_copy(dt, dx, hop, s).start()
        twin_copy(dt, dx, s).start()

    def line_arrived(dist, s):
        for up in (True, False):
            q = r - dist if up else r + dist
            ok = (q >= 0) if up else (q < R)

            @pl.when(ok)
            def _():
                line_copy(line.at[q, s], q, s, up).wait_recv()
                send_line(line.at[q, s], q, s, up)
                send_col(line.at[q, s], q, s)

    own_out = pltpu.make_async_copy(x_ref, rows_ref.at[pl.ds(pl.multiple_of(t * half, 8), half),
                                                       pl.ds(pl.multiple_of(c * width, width), width)], local_sem)
    for s in range(S):
        send_line(part(s), r, s, True)
        send_line(part(s), r, s, False)
    for s in range(S):
        for i in range(len(near)):
            own_copy(i, s).start()
    for s in range(S):
        own_twin(s).start()
        send_col(part(s), r, s)
    own_out.start()

    for dist in range(1, R):
        for s in range(S):
            line_arrived(dist, s)
            if dist == min(2, R - 1) and s == S - 1:
                for s2 in range(S):
                    for dt, dx in near:
                        row_arrived(dt, dx, s2)
            if dist == min(2, R - 1):
                for dt, dx in far:
                    row_arrived(dt, dx, s)

    own_out.wait()
    for s in range(S):
        for i in range(len(near)):
            own_copy(i, s).wait_send()
        own_twin(s).wait_send()
        own_twin_slot = row_slot(t, twin, s)
        rdma(own_twin_slot, own_twin_slot, row_send.at[len(near), s], row_recv.at[t, twin, s], to(t, r, twin)).wait_recv()
        for dt, dx in near + far:
            twin_copy(dt, dx, s).wait_send()
            tt, cc = at_chip(-dt, -dx)
            theirs = row_slot(tt, cc + 1 - 2 * core, s)
            rdma(theirs, theirs, twin_send.at[dt, dx, s], row_recv.at[tt, cc + 1 - 2 * core, s], to(t, r, twin)).wait_recv()
    for s in range(S):
        for tt in range(T):
            for j in range(n):
                slot = col_slot(tt, j, s)
                pltpu.make_async_copy(slot, slot, col_recv.at[tt, j, s]).wait()
        for q in range(R):
            tt, cc, j = col_place(q)

            @pl.when(jnp.logical_not(jnp.logical_and(tt == t, cc == c)))
            def _():
                col_copy(part(s), q, s).wait_send()

            @pl.when(jnp.logical_and(q <= r, r < R - 1))
            def _():
                line_copy(part(s), q, s, True).wait_send()

            @pl.when(jnp.logical_and(q >= r, r > 0))
            def _():
                line_copy(part(s), q, s, False).wait_send()


def gather(returns, T, R, C, S=2):
    half, width = returns.shape
    n = R // T
    S = S if width % (128 * S) == 0 else 1
    sub = width // S
    dma = pltpu.SemaphoreType.DMA
    chips = C // 2
    near = T * chips - 1
    dt = returns.dtype
    return pl.pallas_call(
        functools.partial(gather_kernel, T, R, C, S),
        out_shape=(
            jax.ShapeDtypeStruct((T * half, C * width), dt),
            jax.ShapeDtypeStruct((T * half, n * width), dt),
        ),
        in_specs=[pl.BlockSpec(memory_space=pltpu.VMEM)],
        out_specs=(pl.BlockSpec(memory_space=pl.ANY), pl.BlockSpec(memory_space=pl.ANY)),
        scratch_shapes=[
            pltpu.VMEM((R, S, half, sub), dt),
            dma((2, R, S)), dma((R, S)),
            dma((near + 1, S)), dma((T, C, S)), dma((T, chips, S)), dma((T, chips, max(T, chips), S)),
            dma((R, S)), dma((T, n, S)), dma,
        ],
        compiler_params=pltpu.CompilerParams(collective_id=0, has_side_effects=True),
    )(returns)


DEPTH = 256
FOLD = 6
BF = jnp.bfloat16
F32 = jnp.float32


def split3(v):
    hi = v.astype(BF).astype(F32)
    mid = (v - hi).astype(BF).astype(F32)
    return hi, mid, v - hi - mid


def indicator(cond):
    return jnp.where(cond, 1.0, 0.0).astype(BF)


def wide_mask(m, width):
    return jnp.concatenate([m] * (width // 128), axis=1)


def corr_kernel(tile, chunk, window_ref, days_ref, rows_hbm, cols_hbm, out_ref,
                row_ref, col_ref, mask_ref, head_a, rest_a, head_b, rest_b,
                row_stat, row_p, col_head, col_a, col_m, obuf, sems, load_sems):
    K = days_ref.shape[0]
    days, M = row_ref.shape
    N = col_ref.shape[1]
    extra = days - DEPTH
    heads = 128 // 16
    w = window_ref[0]
    wide = w.astype(F32)
    recip = 1.0 / wide
    fold = w <= DEPTH - FOLD
    load_cols = pltpu.make_async_copy(cols_hbm, col_ref, load_sems.at[0])
    load_rows = pltpu.make_async_copy(rows_hbm, row_ref, load_sems.at[1])
    load_cols.start()
    load_rows.start()

    kk = lax.broadcasted_iota(jnp.int32, (16, days), 0)
    day = lax.broadcasted_iota(jnp.int32, (16, days), 1)
    lasts = jnp.full((16, days), -1, jnp.int32)
    for k in range(K):
        lasts = jnp.where(kk == k, days_ref[k], lasts)
    inside = indicator((day <= lasts) & (day > lasts - w))

    slot = lax.broadcasted_iota(jnp.int32, (16, 128), 0)
    folded_blocks = (extra + FOLD - 1) // 16 + 1

    for k in range(K):
        last = days_ref[k]
        for blk in range(heads):
            s = slot + 16 * blk
            keep = s > last - w
            if blk == 0:
                keep = keep & (s + DEPTH > last)
            mask_ref[k, blk] = indicator(keep)
        mask_ref[k, heads] = indicator(slot + DEPTH <= last)
        for blk in range(folded_blocks):
            n = slot + 16 * blk - (last - (DEPTH - 1))
            sets = ((0, 1, 4), (2, 3), (5,), (0, 2, 5), (1, 3), (4,))
            for e, members in enumerate(sets):
                hit = functools.reduce(jnp.logical_or, [n == v for v in members])
                mask_ref[k, heads + 1 + 6 * blk + e] = indicator(fold & hit)

    def stats(x):
        xf = x.astype(F32)
        sq = xf * xf
        hi = sq.astype(BF)
        lo = (sq - hi.astype(F32)).astype(BF)
        dot = functools.partial(jnp.dot, preferred_element_type=F32)
        first = dot(inside, x)
        second = dot(inside, hi) + dot(inside, lo)
        scale = lax.rsqrt((second - first * first / wide) / wide + 1e-06)
        return first, scale

    def head_of(k, x, value, side):
        width = x.shape[1]
        parts = [jnp.broadcast_to(p[k:k + 1], (16, width)).astype(BF) for p in value]
        blocks = []
        for blk in range(heads):
            v = x[16 * blk:16 * blk + 16] * wide_mask(mask_ref[k, blk], width)
            if blk == 0:
                v = v + x[DEPTH:] * wide_mask(mask_ref[k, heads], width)
            if blk < folded_blocks:
                for e, p in enumerate(parts):
                    v = v + p * wide_mask(mask_ref[k, heads + 1 + 6 * blk + 3 * side + e], width)
            blocks.append(v)
        return jnp.concatenate(blocks, axis=0)

    load_cols.wait()
    for c0 in range(0, N, chunk):
        at = pl.ds(c0, chunk)
        x = col_ref[:, at]
        first, scale = stats(x)
        a = scale * recip
        m = first * recip * a
        parts = split3(first)
        for k in range(K):
            col_a[k, :, at] = a[k:k + 1]
            col_m[k, :, at] = m[k:k + 1]
            col_head[k, :, at] = head_of(k, x, parts, 1)
    load_rows.wait()

    for c0 in range(0, M, chunk):
        at = pl.ds(c0, chunk)
        first, scale = stats(row_ref[:, at])
        row_p[:, at] = (-first * recip)[:8]
        both = jnp.concatenate([scale[:8], (first * scale)[:8]], axis=0)
        row_stat[at, :] = jnp.concatenate([both, jnp.zeros((112, chunk), F32)], axis=0).T

    def prepare(i, refs):
        head, rest = refs
        at = pl.ds(pl.multiple_of(i * tile, tile), tile)
        x = row_ref[:, at]
        parts = split3(row_p[:, at])
        for k in range(K):
            head[k] = head_of(k, x, parts, 0).T
            if k == K - 1:
                rest[...] = x[128:DEPTH].T
            yield

    step = 256 if N % 256 == 0 else 128
    G = M // tile

    span = N // 2 if N % (2 * step) == 0 else N
    pieces = range(N // span)

    def copy_out(i, b, k, h):
        at = pl.ds(h * span, span)
        return pltpu.make_async_copy(obuf.at[b, k, :, at],
                                     out_ref.at[k, pl.ds(pl.multiple_of(i * tile, tile), tile), at],
                                     sems.at[b, k, h])

    def multiply(i, b, refs, folded, stages):
        head, rest = refs
        at = pl.ds(pl.multiple_of(i * tile, tile), tile)
        for k in range(K):
            lhs = jnp.concatenate([head[k], rest[...]], axis=1)
            s = jnp.broadcast_to(row_stat[at, k:k + 1], (tile, 128))
            s = jnp.concatenate([s] * (step // 128), axis=1)
            if not folded:
                m = jnp.broadcast_to(row_stat[at, 8 + k:9 + k], (tile, 128))
                m = jnp.concatenate([m] * (step // 128), axis=1)
            for j in range(0, N, step):
                rhs = jnp.concatenate([col_head[k, :, j:j + step], col_ref[128:DEPTH, j:j + step]], axis=0)
                g = jnp.dot(lhs, rhs, preferred_element_type=F32)
                o = (g * s) * col_a[k, :, j:j + step]
                if not folded:
                    o = o - m * col_m[k, :, j:j + step]
                obuf[b, k, :, j:j + step] = o.astype(BF)
                if (j + step) % span == 0:
                    copy_out(i, b, k, j // span).start()
            next(stages, None)
        for _ in stages:
            pass

    first_refs = (head_a, rest_a)
    second_refs = (head_b, rest_b)
    for _ in prepare(0, first_refs):
        pass

    def run(folded):
        def body(p, carry):
            for b, (now, later) in enumerate(((first_refs, second_refs), (second_refs, first_refs))):
                i = 2 * p + b

                @pl.when(p > 0)
                def _():
                    for k in range(K):
                        for h in pieces:
                            copy_out(i - 2, b, k, h).wait()
                multiply(i, b, now, folded, prepare(jnp.minimum(i + 1, G - 1), later))
            return carry

        lax.fori_loop(0, G // 2, body, 0)

    @pl.when(fold)
    def _():
        run(True)

    @pl.when(jnp.logical_not(fold))
    def _():
        run(False)

    for b in range(2):
        for k in range(K):
            for h in pieces:
                copy_out(G - 2 + b, b, k, h).wait()


def correlate(window, out_days, rows, cols, tile=512, chunk=1024):
    days, M = rows.shape
    N = cols.shape[1]
    K = out_days.shape[0]
    tile = min(tile, M // 2)
    chunk = min(chunk, N, M)
    folded_blocks = (days - DEPTH + FOLD - 1) // 16 + 1
    smem = pl.BlockSpec(memory_space=pltpu.SMEM)
    hbm = pl.BlockSpec(memory_space=pl.ANY)
    side = [pltpu.VMEM((K, tile, 128), BF), pltpu.VMEM((tile, 128), BF)]
    return pl.pallas_call(
        functools.partial(corr_kernel, tile, chunk),
        out_shape=jax.ShapeDtypeStruct((K, M, N), BF),
        in_specs=[smem, smem, hbm, hbm],
        out_specs=hbm,
        scratch_shapes=[
            pltpu.VMEM((days, M), BF),
            pltpu.VMEM((days, N), BF),
            pltpu.VMEM((K, 9 + 6 * folded_blocks, 16, 128), BF),
            *side, *side,
            pltpu.VMEM((M, 128), F32),
            pltpu.VMEM((8, M), F32),
            pltpu.VMEM((K, 128, N), BF),
            pltpu.VMEM((K, 1, N), F32),
            pltpu.VMEM((K, 1, N), F32),
            pltpu.VMEM((2, K, tile, N), BF),
            pltpu.SemaphoreType.DMA((2, K, 2)),
            pltpu.SemaphoreType.DMA((2,)),
        ],
        compiler_params=pltpu.CompilerParams(vmem_limit_bytes=60 * 2**20),
    )(window, out_days, rows, cols)


def on_device(returns, window, out_days):
    T, R, C = lax.axis_size("tm"), lax.axis_size("row"), lax.axis_size("col")
    rows, cols = gather(returns, T, R, C)
    return correlate(window, out_days, rows, cols)


def solution(mesh):
    return jax.shard_map(
        on_device,
        mesh=mesh,
        in_specs=(P("tm", ("row", "col")), P(), P()),
        out_specs=P(None, "row", ("col", "tm")),
        check_vma=False,
    )
```
